8 devices in a mesh: rep: 1 (over z), dp: 8 (over x, y, core).
Axes of the slice: x: 2, y: 2, z: 1, core: 2. Of those that a mesh axis runs over, the one named last changes fastest.
Arguments:
- a: bfloat16 [8, 4, 4096, 1280], P(('rep', 'dp'))
- g: bfloat16 [8, 4, 4096, 5120], P(('rep', 'dp'))
Outputs:
- output: bfloat16 [4, 1280, 5120], P('rep')
All inputs are finite; a program needn't handle non-finite values.
Results may differ from the reference program's by a relative error of at most 0.012.
Values are sent between devices in bfloat16 or wider.
A program may use at most 2 GiB of HBM per device.

```python
import jax
import jax.numpy as jnp
from jax import lax

DEVICES = 8
MATRICES = 4
TOKENS = 4096
D = 1280
FF = 5120


def setup_inputs(seed: int = 0, part: int = 0) -> dict:
    ka, kg, ks = (jax.random.fold_in(k, part) for k in jax.random.split(jax.random.key(seed), 3))
    size = 2.0 ** jax.random.uniform(ks, (DEVICES, MATRICES, 1, 1), jnp.float32, -1.0, 1.0)
    a = jax.random.normal(ka, (DEVICES, MATRICES, TOKENS, D), jnp.float32)
    g = size * jax.random.normal(kg, (DEVICES, MATRICES, TOKENS, FF), jnp.float32) * (DEVICES * TOKENS) ** -0.5
    return {"a": a.astype(jnp.bfloat16), "g": g.astype(jnp.bfloat16)}


def reference(a, g):
    def take(so_far, one):
        return so_far + jnp.einsum("ntd,ntf->ndf", *one, preferred_element_type=jnp.float32), None

    return lax.scan(take, jnp.zeros((MATRICES, D, FF), jnp.float32), (a, g))[0].astype(jnp.bfloat16)
```

```python
import functools

import jax
import jax.numpy as jnp
from jax import lax
from jax.experimental import pallas as pl
from jax.experimental.pallas import tpu as pltpu
from jax.sharding import PartitionSpec as P

MESH = pl.DeviceIdType.MESH
ANY = pl.BlockSpec(memory_space=pl.ANY)
F32, BF16 = jnp.float32, jnp.bfloat16


N, T, D, F = 4, 4096, 1280, 5120
C = 256
PER = F // C
UNITS = N * PER
HALF, QUARTER, EIGHTH = D // 2, D // 4, D // 8
LAG1, LAG2, LAG3 = 3, 3, 2
AT1 = 1
AT2 = AT1 + LAG1
AT3 = AT2 + LAG2
AT4 = AT3 + LAG3
TURNS = UNITS + AT4
SLOTS = 8
CHUNKS = [(0, 0, F), (1, 0, F), (2, 0, F), (3, 0, 2560), (3, 2560, 1536), (3, 4096, 1024)]


def place_of():
    r = lax.axis_index("dp")
    x, y, c = r // 4, lax.rem(r // 2, 2), lax.rem(r, 2)
    return x, y, c, x * (1 - c) + y * c, y * (1 - c) + x * c


def index(x, y, c):
    return (x * 2 + y) * 2 + c


def peers():
    x, y, c, _, _ = place_of()
    return (
        index(x, y, 1 - c),
        index(x + (1 - 2 * x) * (1 - c), y + (1 - 2 * y) * c, c),
        index(x + (1 - 2 * x) * c, y + (1 - 2 * y) * (1 - c), c),
    )


def reduce_kernel(a_ref, g_ref, *refs):
    outs = refs[: len(CHUNKS)]
    (abuf, gbuf, acc, send0, recv0, send1, recv1, send2, recv2, done,
     a_sem, g_sem, s0, r0, s1, r1, s2, r2, s3, r3, w3) = refs[len(CHUNKS):]
    _, _, c, p1, p2 = place_of()
    pair, near1, near2 = peers()

    def a_copy(n):
        return pltpu.make_async_copy(a_ref.at[n], abuf.at[lax.rem(n, 2)], a_sem.at[lax.rem(n, 2)])

    def g_copy(u):
        n, col = u // PER, pl.multiple_of(lax.rem(u, PER) * C, C)
        return pltpu.make_async_copy(g_ref.at[n, :, pl.ds(col, C)], gbuf.at[lax.rem(u, 2)], g_sem.at[lax.rem(u, 2)])

    def remote(src, dst, send, recv, to):
        return pltpu.make_async_remote_copy(src, dst, send, recv, device_id=(0, to), device_id_type=MESH)

    def copy0(u):
        s, t = lax.rem(u, 2), lax.rem(u, SLOTS)
        return remote(send0.at[s], recv0.at[t], s0.at[s], r0.at[t], pair)

    def copy1(u):
        s = lax.rem(u, SLOTS)
        return remote(send1.at[s], recv1.at[s], s1.at[s], r1.at[s], near1)

    def copy2(u):
        s = lax.rem(u, SLOTS)
        return remote(send2.at[s], recv2.at[s], s2.at[s], r2.at[s], near2)

    def finished(u, out, first):
        s = lax.rem(u, SLOTS)
        col = pl.multiple_of((u - first) * C, C)
        dst = out.at[pl.ds(pl.multiple_of(p2 * EIGHTH, EIGHTH), EIGHTH), pl.ds(col, C)]
        return remote(done.at[s], dst, s3.at[s], r3.at[s], near2), pltpu.make_async_copy(done.at[s], dst, w3.at[s])

    a_copy(0).start()
    g_copy(0).start()
    barrier = pltpu.get_barrier_semaphore()
    for to in (pair, near1, near2):
        pl.semaphore_signal(barrier, 1, device_id=(0, to), device_id_type=MESH)
    pl.semaphore_wait(barrier, 3)

    def rows(k, size):
        return pl.ds(pl.multiple_of(k * size, size), size)

    def turn(i, _):
        @pl.when(i < UNITS)
        def _():
            n = i // PER

            @pl.when(i + 1 < UNITS)
            def _():
                g_copy(i + 1).start()

            @pl.when(lax.rem(i, PER) == 0)
            def _():
                a_copy(n).wait()

                @pl.when(n + 1 < N)
                def _():
                    a_copy(n + 1).start()

            g_copy(i).wait()
            s = lax.rem(i, SLOTS + 1)
            acc[s] = lax.dot_general(
                abuf[lax.rem(n, 2)], gbuf[lax.rem(i, 2)], (((0,), (0,)), ((), ())), preferred_element_type=F32
            )

            @pl.when(i >= 2)
            def _():
                copy0(i - 2).wait_send()

            send0[lax.rem(i, 2)] = acc[s, rows(1 - c, HALF), :].astype(BF16)
            copy0(i).start()

        @pl.when((i >= AT1) & (i < UNITS + AT1))
        def _():
            u = i - AT1
            s, t = lax.rem(u, SLOTS + 1), lax.rem(u, SLOTS)
            copy0(u).wait_recv()

            @pl.when(u >= SLOTS)
            def _():
                copy1(u - SLOTS).wait_send()

            away, keep = rows(1 - p1, QUARTER), rows(p1, QUARTER)
            mine = c * 2
            send1[t] = (acc[s, rows(mine + 1 - p1, QUARTER), :] + recv0[t, away, :].astype(F32)).astype(BF16)
            copy1(u).start()
            acc[s, rows(mine + p1, QUARTER), :] = acc[s, rows(mine + p1, QUARTER), :] + recv0[t, keep, :].astype(F32)

        @pl.when((i >= AT2) & (i < UNITS + AT2))
        def _():
            u = i - AT2
            s, t = lax.rem(u, SLOTS + 1), lax.rem(u, SLOTS)
            copy1(u).wait_recv()

            @pl.when(u >= SLOTS)
            def _():
                copy2(u - SLOTS).wait_send()

            mine = (c * 2 + p1) * 2
            send2[t] = (
                acc[s, rows(mine + 1 - p2, EIGHTH), :] + recv1[t, rows(1 - p2, EIGHTH), :].astype(F32)
            ).astype(BF16)
            copy2(u).start()
            acc[s, rows(mine + p2, EIGHTH), :] = (
                acc[s, rows(mine + p2, EIGHTH), :] + recv1[t, rows(p2, EIGHTH), :].astype(F32)
            )

        @pl.when((i >= AT3) & (i < UNITS + AT3))
        def _():
            u = i - AT3
            s, t = lax.rem(u, SLOTS + 1), lax.rem(u, SLOTS)
            copy2(u).wait_recv()
            mine = (c * 2 + p1) * 2 + p2
            done[t] = (acc[s, rows(mine, EIGHTH), :] + recv2[t].astype(F32)).astype(BF16)
            for (n, col, width), out in zip(CHUNKS, outs):
                first = n * PER + col // C

                @pl.when((u >= first) & (u < first + width // C))
                def _(out=out, first=first):
                    there, here = finished(u, out, first)
                    there.start()
                    here.start()

        @pl.when(i >= AT4)
        def _():
            u = i - AT4
            there, here = finished(u, outs[0], u)
            there.wait_recv()
            there.wait_send()
            here.wait()

        return 0

    lax.fori_loop(0, TURNS, turn, 0)
    for k in range(2):
        copy0(UNITS - 2 + k).wait_send()
    for k in range(SLOTS):
        copy1(UNITS - SLOTS + k).wait_send()
        copy2(UNITS - SLOTS + k).wait_send()


def reduce_call(a, g):
    dma = pltpu.SemaphoreType.DMA
    return pl.pallas_call(
        reduce_kernel,
        name="reduce",
        out_shape=[jax.ShapeDtypeStruct((QUARTER, width), BF16) for _, _, width in CHUNKS],
        in_specs=[ANY] * 2,
        out_specs=[ANY] * len(CHUNKS),
        scratch_shapes=[
            pltpu.VMEM((2, T, D), BF16),
            pltpu.VMEM((2, T, C), BF16),
            pltpu.VMEM((SLOTS + 1, D, C), F32),
            pltpu.VMEM((2, HALF, C), BF16),
            pltpu.VMEM((SLOTS, HALF, C), BF16),
            pltpu.VMEM((SLOTS, QUARTER, C), BF16),
            pltpu.VMEM((SLOTS, QUARTER, C), BF16),
            pltpu.VMEM((SLOTS, EIGHTH, C), BF16),
            pltpu.VMEM((SLOTS, EIGHTH, C), BF16),
            pltpu.VMEM((SLOTS, EIGHTH, C), BF16),
            dma((2,)), dma((2,)), dma((2,)), dma((SLOTS,)),
            dma((SLOTS,)), dma((SLOTS,)), dma((SLOTS,)), dma((SLOTS,)),
            dma((SLOTS,)), dma((SLOTS,)), dma((SLOTS,)),
        ],
        compiler_params=pltpu.CompilerParams(
            collective_id=0, has_side_effects=True, vmem_limit_bytes=62 * 2**20
        ),
        cost_estimate=pl.CostEstimate(flops=2 * N * T * D * F, transcendentals=0, bytes_accessed=N * T * (D + F) * 2),
    )(a, g)


def put_kernel(n, col, width, kinds, tile, *refs):
    srcs, out, (buf, si, so) = refs[: len(kinds)], refs[-4], refs[-3:]
    _, _, c, p1, p2 = place_of()
    block = {"X": 2 * c + p1, "Y": 2 * c + 1 - p1, "XP": 2 * (1 - c) + p2, "YP": 2 * (1 - c) + 1 - p2}
    pieces = [(src, kind, t) for src, kind in zip(srcs, kinds) for t in range(QUARTER // tile)]
    depth = buf.shape[0]

    def load(i):
        src, _, t = pieces[i]
        return pltpu.make_async_copy(src.at[pl.ds(t * tile, tile)], buf.at[i % depth], si.at[i % depth])

    def store(i):
        _, kind, t = pieces[i]
        row = pl.multiple_of(block[kind] * QUARTER + t * tile, 16)
        return pltpu.make_async_copy(
            buf.at[i % depth], out.at[n, pl.ds(row, tile), pl.ds(col, width)], so.at[i % depth]
        )

    ahead, count = depth // 2, len(pieces)
    for i in range(min(ahead, count)):
        load(i).start()
    for i in range(count):
        load(i).wait()
        store(i).start()
        j = i + ahead
        if j < count:
            if j >= depth:
                store(j - depth).wait()
            load(j).start()
    for i in range(max(0, count - depth), count):
        store(i).wait()


def put(out, chunk, **srcs):
    n, col, width = chunk
    kinds, arrays = tuple(srcs), list(srcs.values())
    tile, depth = (160 if width > 2560 else 320), 4
    args = arrays + ([] if out is None else [out])
    return pl.pallas_call(
        functools.partial(put_kernel, n, col, width, kinds, tile),
        name=f"put_{n}_{col}_" + "_".join(kinds),
        out_shape=jax.ShapeDtypeStruct((N, D, F), BF16),
        in_specs=[ANY] * len(args),
        out_specs=ANY,
        scratch_shapes=[
            pltpu.VMEM((depth, tile, width), BF16), pltpu.SemaphoreType.DMA((depth,)), pltpu.SemaphoreType.DMA((depth,))
        ],
        input_output_aliases={} if out is None else {len(arrays): 0},
        cost_estimate=pl.CostEstimate(flops=0, transcendentals=0, bytes_accessed=len(arrays) * QUARTER * width * 4),
        compiler_params=pltpu.CompilerParams(vmem_limit_bytes=40 * 2**20),
    )(*args)


def solution(mesh):
    places = [(x, y, c) for x in (0, 1) for y in (0, 1) for c in (0, 1)]
    along = [(index(x, y, c), index(1 - x, y, c) if c == 0 else index(x, 1 - y, c)) for x, y, c in places]
    across = [(index(x, y, c), index(x, y, 1 - c)) for x, y, c in places]

    def step(a, g):
        blocks = list(reduce_call(a[0], g[0]))
        out, count = None, len(CHUNKS)
        ys, xps, yps = [None] * count, [None] * count, [None] * count
        for k in range(count + 2):
            if k < count:
                x = blocks[k]
                if out is not None:
                    x, out = lax.optimization_barrier((x, out))
                blocks[k] = x
                ys[k] = lax.ppermute(x, "dp", along)
                xps[k] = lax.ppermute(x, "dp", across)
            if 1 <= k <= count:
                j = k - 1
                out = put(out, CHUNKS[j], X=blocks[j], XP=xps[j])
            if 2 <= k:
                j = k - 2
                yps[j] = lax.ppermute(ys[j], "dp", across)
                out = put(out, CHUNKS[j], Y=ys[j], YP=yps[j])
        return out

    return jax.shard_map(
        step, mesh=mesh, in_specs=(P(("rep", "dp")), P(("rep", "dp"))), out_specs=P("rep", None, None), check_vma=False
    )
```

```python
import functools

import jax
import jax.numpy as jnp
from jax import lax
from jax.experimental import pallas as pl
from jax.experimental.pallas import tpu as pltpu
from jax.sharding import PartitionSpec as P


MESH = pl.DeviceIdType.MESH
ANY = pl.BlockSpec(memory_space=pl.ANY)
F32, BF16 = jnp.float32, jnp.bfloat16


N, T, D, F = 4, 4096, 1280, 5120
C = 256
PER = F // C
UNITS = N * PER
HALF, QUARTER, EIGHTH = D // 2, D // 4, D // 8
LAG1, LAG2, LAG3 = 3, 3, 2
AT1 = 1
AT2 = AT1 + LAG1
AT3 = AT2 + LAG2
AT4 = AT3 + LAG3
TURNS = UNITS + AT4
SLOTS = 8
CHUNKS = [(0, 0, F), (1, 0, F), (2, 0, F), (3, 0, 2560), (3, 2560, 1536), (3, 4096, 1024)]


def place_of():
    r = lax.axis_index("dp")
    x, y, c = r // 4, lax.rem(r // 2, 2), lax.rem(r, 2)
    return x, y, c, x * (1 - c) + y * c, y * (1 - c) + x * c


def index(x, y, c):
    return (x * 2 + y) * 2 + c


def peers():
    x, y, c, _, _ = place_of()
    return (
        index(x, y, 1 - c),
        index(x + (1 - 2 * x) * (1 - c), y + (1 - 2 * y) * c, c),
        index(x + (1 - 2 * x) * c, y + (1 - 2 * y) * (1 - c), c),
    )


def reduce_kernel(a_ref, g_ref, *refs):
    outs = refs[: len(CHUNKS)]
    (abuf, gbuf, acc, send0, recv0, send1, recv1, send2, recv2, done,
     a_sem, g_sem, s0, r0, s1, r1, s2, r2, s3, r3, w3) = refs[len(CHUNKS):]
    _, _, c, p1, p2 = place_of()
    pair, near1, near2 = peers()

    def a_copy(n):
        return pltpu.make_async_copy(a_ref.at[n], abuf.at[lax.rem(n, 2)], a_sem.at[lax.rem(n, 2)])

    def g_copy(u):
        n, col = u // PER, pl.multiple_of(lax.rem(u, PER) * C, C)
        return pltpu.make_async_copy(g_ref.at[n, :, pl.ds(col, C)], gbuf.at[lax.rem(u, 2)], g_sem.at[lax.rem(u, 2)])

    def remote(src, dst, send, recv, to):
        return pltpu.make_async_remote_copy(src, dst, send, recv, device_id=(0, to), device_id_type=MESH)

    def copy0(u):
        s, t = lax.rem(u, 2), lax.rem(u, SLOTS)
        return remote(send0.at[s], recv0.at[t], s0.at[s], r0.at[t], pair)

    def copy1(u):
        s = lax.rem(u, SLOTS)
        return remote(send1.at[s], recv1.at[s], s1.at[s], r1.at[s], near1)

    def copy2(u):
        s = lax.rem(u, SLOTS)
        return remote(send2.at[s], recv2.at[s], s2.at[s], r2.at[s], near2)

    def finished(u, out, first):
        s = lax.rem(u, SLOTS)
        col = pl.multiple_of((u - first) * C, C)
        dst = out.at[pl.ds(pl.multiple_of(p2 * EIGHTH, EIGHTH), EIGHTH), pl.ds(col, C)]
        return remote(done.at[s], dst, s3.at[s], r3.at[s], near2), pltpu.make_async_copy(done.at[s], dst, w3.at[s])

    a_copy(0).start()
    g_copy(0).start()
    barrier = pltpu.get_barrier_semaphore()
    for to in (pair, near1, near2):
        pl.semaphore_signal(barrier, 1, device_id=(0, to), device_id_type=MESH)
    pl.semaphore_wait(barrier, 3)

    def rows(k, size):
        return pl.ds(pl.multiple_of(k * size, size), size)

    def turn(i, _):
        @pl.when(i < UNITS)
        def _():
            n = i // PER

            @pl.when(i + 1 < UNITS)
            def _():
                g_copy(i + 1).start()

            @pl.when(lax.rem(i, PER) == 0)
            def _():
                a_copy(n).wait()

                @pl.when(n + 1 < N)
                def _():
                    a_copy(n + 1).start()

            g_copy(i).wait()
            s = lax.rem(i, SLOTS + 1)
            acc[s] = lax.dot_general(
                abuf[lax.rem(n, 2)], gbuf[lax.rem(i, 2)], (((0,), (0,)), ((), ())), preferred_element_type=F32
            )

            @pl.when(i >= 2)
            def _():
                copy0(i - 2).wait_send()

            send0[lax.rem(i, 2)] = acc[s, rows(1 - c, HALF), :].astype(BF16)
            copy0(i).start()

        @pl.when((i >= AT1) & (i < UNITS + AT1))
        def _():
            u = i - AT1
            s, t = lax.rem(u, SLOTS + 1), lax.rem(u, SLOTS)
            copy0(u).wait_recv()

            @pl.when(u >= SLOTS)
            def _():
                copy1(u - SLOTS).wait_send()

            away, keep = rows(1 - p1, QUARTER), rows(p1, QUARTER)
            mine = c * 2
            send1[t] = (acc[s, rows(mine + 1 - p1, QUARTER), :] + recv0[t, away, :].astype(F32)).astype(BF16)
            copy1(u).start()
            acc[s, rows(mine + p1, QUARTER), :] = acc[s, rows(mine + p1, QUARTER), :] + recv0[t, keep, :].astype(F32)

        @pl.when((i >= AT2) & (i < UNITS + AT2))
        def _():
            u = i - AT2
            s, t = lax.rem(u, SLOTS + 1), lax.rem(u, SLOTS)
            copy1(u).wait_recv()

            @pl.when(u >= SLOTS)
            def _():
                copy2(u - SLOTS).wait_send()

            mine = (c * 2 + p1) * 2
            send2[t] = (
                acc[s, rows(mine + 1 - p2, EIGHTH), :] + recv1[t, rows(1 - p2, EIGHTH), :].astype(F32)
            ).astype(BF16)
            copy2(u).start()
            acc[s, rows(mine + p2, EIGHTH), :] = (
                acc[s, rows(mine + p2, EIGHTH), :] + recv1[t, rows(p2, EIGHTH), :].astype(F32)
            )

        @pl.when((i >= AT3) & (i < UNITS + AT3))
        def _():
            u = i - AT3
            s, t = lax.rem(u, SLOTS + 1), lax.rem(u, SLOTS)
            copy2(u).wait_recv()
            mine = (c * 2 + p1) * 2 + p2
            done[t] = (acc[s, rows(mine, EIGHTH), :] + recv2[t].astype(F32)).astype(BF16)
            for (n, col, width), out in zip(CHUNKS, outs):
                first = n * PER + col // C

                @pl.when((u >= first) & (u < first + width // C))
                def _(out=out, first=first):
                    there, here = finished(u, out, first)
                    there.start()
                    here.start()

        @pl.when(i >= AT4)
        def _():
            u = i - AT4
            there, here = finished(u, outs[0], u)
            there.wait_recv()
            there.wait_send()
            here.wait()

        return 0

    lax.fori_loop(0, TURNS, turn, 0)
    for k in range(2):
        copy0(UNITS - 2 + k).wait_send()
    for k in range(SLOTS):
        copy1(UNITS - SLOTS + k).wait_send()
        copy2(UNITS - SLOTS + k).wait_send()


def reduce_call(a, g):
    dma = pltpu.SemaphoreType.DMA
    return pl.pallas_call(
        reduce_kernel,
        name="reduce",
        out_shape=[jax.ShapeDtypeStruct((QUARTER, width), BF16) for _, _, width in CHUNKS],
        in_specs=[ANY] * 2,
        out_specs=[ANY] * len(CHUNKS),
        scratch_shapes=[
            pltpu.VMEM((2, T, D), BF16),
            pltpu.VMEM((2, T, C), BF16),
            pltpu.VMEM((SLOTS + 1, D, C), F32),
            pltpu.VMEM((2, HALF, C), BF16),
            pltpu.VMEM((SLOTS, HALF, C), BF16),
            pltpu.VMEM((SLOTS, QUARTER, C), BF16),
            pltpu.VMEM((SLOTS, QUARTER, C), BF16),
            pltpu.VMEM((SLOTS, EIGHTH, C), BF16),
            pltpu.VMEM((SLOTS, EIGHTH, C), BF16),
            pltpu.VMEM((SLOTS, EIGHTH, C), BF16),
            dma((2,)), dma((2,)), dma((2,)), dma((SLOTS,)),
            dma((SLOTS,)), dma((SLOTS,)), dma((SLOTS,)), dma((SLOTS,)),
            dma((SLOTS,)), dma((SLOTS,)), dma((SLOTS,)),
        ],
        compiler_params=pltpu.CompilerParams(
            collective_id=0, has_side_effects=True, vmem_limit_bytes=62 * 2**20
        ),
        cost_estimate=pl.CostEstimate(flops=2 * N * T * D * F, transcendentals=0, bytes_accessed=N * T * (D + F) * 2),
    )(a, g)


def put_kernel(n, col, width, kinds, tile, *refs):
    srcs, out, (buf, si, so) = refs[: len(kinds)], refs[-4], refs[-3:]
    _, _, c, p1, p2 = place_of()
    block = {"X": 2 * c + p1, "Y": 2 * c + 1 - p1, "XP": 2 * (1 - c) + p2, "YP": 2 * (1 - c) + 1 - p2}
    pieces = [(src, kind, t) for src, kind in zip(srcs, kinds) for t in range(QUARTER // tile)]
    depth = buf.shape[0]

    def load(i):
        src, _, t = pieces[i]
        return pltpu.make_async_copy(src.at[pl.ds(t * tile, tile)], buf.at[i % depth], si.at[i % depth])

    def store(i):
        _, kind, t = pieces[i]
        row = pl.multiple_of(block[kind] * QUARTER + t * tile, 16)
        return pltpu.make_async_copy(
            buf.at[i % depth], out.at[n, pl.ds(row, tile), pl.ds(col, width)], so.at[i % depth]
        )

    ahead, count = depth // 2, len(pieces)
    for i in range(min(ahead, count)):
        load(i).start()
    for i in range(count):
        load(i).wait()
        store(i).start()
        j = i + ahead
        if j < count:
            if j >= depth:
                store(j - depth).wait()
            load(j).start()
    for i in range(max(0, count - depth), count):
        store(i).wait()


def put(out, chunk, **srcs):
    n, col, width = chunk
    kinds, arrays = tuple(srcs), list(srcs.values())
    tile, depth = (160 if width > 2560 else 320), 4
    args = arrays + ([] if out is None else [out])
    return pl.pallas_call(
        functools.partial(put_kernel, n, col, width, kinds, tile),
        out_shape=jax.ShapeDtypeStruct((N, D, F), BF16),
        in_specs=[ANY] * len(args),
        out_specs=ANY,
        scratch_shapes=[
            pltpu.VMEM((depth, tile, width), BF16), pltpu.SemaphoreType.DMA((depth,)), pltpu.SemaphoreType.DMA((depth,))
        ],
        input_output_aliases={} if out is None else {len(arrays): 0},
        cost_estimate=pl.CostEstimate(flops=0, transcendentals=0, bytes_accessed=len(arrays) * QUARTER * width * 4),
        compiler_params=pltpu.CompilerParams(vmem_limit_bytes=40 * 2**20),
    )(*args)


def solution(mesh):
    places = [(x, y, c) for x in (0, 1) for y in (0, 1) for c in (0, 1)]
    along = [(index(x, y, c), index(1 - x, y, c) if c == 0 else index(x, 1 - y, c)) for x, y, c in places]
    across = [(index(x, y, c), index(x, y, 1 - c)) for x, y, c in places]

    def step(a, g):
        blocks = reduce_call(a[0], g[0])
        ys, xps, yps = [], [], []
        for x in blocks:
            ys.append(lax.ppermute(x, "dp", along))
            xps.append(lax.ppermute(x, "dp", across))
        for y in ys:
            yps.append(lax.ppermute(y, "dp", across))
        out = None
        for k, chunk in enumerate(CHUNKS):
            out = put(out, chunk, X=blocks[k], XP=xps[k])
        for k, chunk in enumerate(CHUNKS):
            out = put(out, chunk, Y=ys[k], YP=yps[k])
        return out

    return jax.shard_map(
        step, mesh=mesh, in_specs=(P(("rep", "dp")), P(("rep", "dp"))), out_specs=P("rep", None, None), check_vma=False
    )
```
